32 devices in a mesh: dp: 2 (over y), pipe: 4 (over x, core), tensor: 4 (over z).
Axes of the slice: x: 2, y: 2, z: 4, core: 2. Of those that a mesh axis runs over, the one named last changes fastest.
Arguments:
- query_states: bfloat16 [4, 512, 1024], P('dp'), may hold values from -6 to 6
- doc_states: bfloat16 [4, 512, 1024], P('dp'), may hold values from -6 to 6
- query_len: int32 [4], P('dp'), may hold values from 64 to 512
- doc_len: int32 [4], P('dp'), may hold values from 64 to 512
- doc_order: int32 [2, 2], P('dp'), may hold values from 0 to 1, each once within a row
- w_qkv: bfloat16 [4, 3, 1024, 1024], P('pipe', None, None, 'tensor'), may hold values from -0.1875 to 0.1875
- w_out: bfloat16 [4, 1024, 1024], P('pipe', 'tensor'), may hold values from -0.1875 to 0.1875
- w_up: bfloat16 [4, 1024, 4096], P('pipe', None, 'tensor'), may hold values from -0.1875 to 0.1875
- w_down: bfloat16 [4, 4096, 1024], P('pipe', 'tensor'), may hold values from -0.09375 to 0.09375
- gain_attn: float32 [4, 1024], P('pipe'), may hold values from 0.1 to 1.9
- gain_mlp: float32 [4, 1024], P('pipe'), may hold values from 0.1 to 1.9
Outputs:
- query_vectors: bfloat16 [4, 1024], P('dp', ('pipe', 'tensor'))
- document_vectors: bfloat16 [4, 1024], P('dp', ('pipe', 'tensor'))
- pair_loss: float32 [4], P('dp')
The draws below stay inside these ranges and needn't reach their ends.
Inputs may be any that keep to these rules, and one draw needn't show every extreme that they name: `doc_order`: each row holds every number of 0 to 1 once.
All inputs are finite; a program needn't handle non-finite values.
Results may differ from the reference program's by a relative error of at most 0.035.
Values may be sent and summed in bfloat16 or wider, within the bound.
No kernel may reach another device: no remote copies, remote signals or barrier semaphores. Data moves between devices by JAX's collectives and lax.ppermute only.
A program may use at most 192 MiB of HBM per device.

```python
import math
import jax
import jax.numpy as jnp
from jax import lax

D = 1024
HEADS = 16
FF = 4096
S = 512
PAIRS_DEV = 2
LAYERS = 4
QUERIES = 4
DOCS = 4
N_DP = 2
N_TENSOR = 4


def set_ends(values, stream_key, low, high):
    longest = values.shape.index(max(values.shape))
    spots = []
    for shift in (0, 1):
        where = [jax.random.randint(jax.random.fold_in(stream_key, axis), (), 0, length) for axis, length in enumerate(values.shape)]
        where[longest] = (where[longest] + shift) % values.shape[longest]
        spots.append(tuple(where))
    return values.at[spots[0]].set(low).at[spots[1]].set(high)


def levels(stream_key, shape, split, low, top_value):
    loudness = 1.0
    for dim, parts in split:
        heights = jax.random.uniform(jax.random.fold_in(jax.random.fold_in(stream_key, 6), dim), (parts,), jnp.float32, low / len(split), top_value / len(split))
        loudness = loudness * jnp.repeat(jnp.exp(heights), shape[dim] // parts).reshape((-1,) + (1,) * (len(shape) - 1 - dim))
    return loudness


def centred(key, dims, spread, limit, split=(), kind=jnp.bfloat16):
    entries = spread * jax.random.normal(key, dims, jnp.float32)
    if split:
        entries = entries * levels(key, dims, split, -0.22, 0.18)
    return jnp.clip(entries, -limit, limit).astype(kind)


def setup_inputs(seed: int = 0) -> dict:
    arg_keys = jax.random.split(jax.random.key(seed), 12)
    query_states = centred(arg_keys[0], (QUERIES, S, D), 1.0, 6.0, ((0, 2),))
    doc_states = centred(arg_keys[1], (DOCS, S, D), 1.0, 6.0, ((0, 2),))
    query_len = set_ends(jax.random.randint(arg_keys[2], (QUERIES,), S // 8, S + 1), jax.random.fold_in(arg_keys[2], 1), S // 8, S).astype(jnp.int32)
    doc_len = set_ends(jax.random.randint(arg_keys[3], (DOCS,), S // 8, S + 1), jax.random.fold_in(arg_keys[3], 1), S // 8, S).astype(jnp.int32)
    doc_order = jax.vmap(lambda own: jax.random.permutation(own, PAIRS_DEV))(jax.random.split(arg_keys[4], N_DP)).reshape((N_DP, PAIRS_DEV)).astype(jnp.int32)
    w_qkv = centred(arg_keys[5], (LAYERS, 3, D, D), D ** -0.5, 0.1875, ((0, 4), (3, 4)))
    w_out = centred(arg_keys[6], (LAYERS, D, D), D ** -0.5, 0.1875, ((0, 4), (1, 4)))
    w_up = centred(arg_keys[7], (LAYERS, D, FF), D ** -0.5, 0.1875, ((0, 4), (2, 4)))
    w_down = centred(arg_keys[8], (LAYERS, FF, D), FF ** -0.5, 0.09375, ((0, 4), (1, 4)))
    gain_attn = jnp.clip(1.0 + 0.18 * jax.random.normal(arg_keys[9], (LAYERS, D), jnp.float32), 0.1, 1.9)
    gain_mlp = jnp.clip(1.0 + 0.18 * jax.random.normal(arg_keys[10], (LAYERS, D), jnp.float32), 0.1, 1.9)
    return {"query_states": query_states, "doc_states": doc_states, "query_len": query_len, "doc_len": doc_len, "doc_order": doc_order, "w_qkv": w_qkv, "w_out": w_out, "w_up": w_up, "w_down": w_down, "gain_attn": gain_attn, "gain_mlp": gain_mlp}


SOFTMAX_TEMPER = 0.05
EPSILON = 1e-06
LAYER_EPSILON = 1e-12

def norm_rows(values_in, gain_row):
    row_mean = lax.optimization_barrier(jnp.mean(values_in, axis=-1, keepdims=True))
    centered = values_in - row_mean
    variance = lax.optimization_barrier(jnp.mean(centered * centered, axis=-1, keepdims=True))
    return centered * lax.rsqrt(variance + LAYER_EPSILON) * gain_row

def group_sum(left_side, right_side):
    row_total = left_side.shape[0]
    group_width = left_side.shape[1] // N_TENSOR
    left_parts = left_side.reshape(row_total, N_TENSOR, group_width).astype(jnp.float32)
    right_parts = right_side.reshape(N_TENSOR, group_width, right_side.shape[1]).astype(jnp.float32)
    partials = jnp.einsum('sgk,gkd->gsd', left_parts, right_parts)
    rounded = lax.optimization_barrier(partials.astype(jnp.bfloat16))
    return lax.optimization_barrier(jnp.sum(rounded.astype(jnp.float32), axis=0))

def encode_layer(hidden, valid_keys, w_qkv, w_out, w_up, w_down, gain_attn, gain_mlp):
    head_width = D // HEADS
    slot_count = hidden.shape[0]
    inv_sqrt = 1.0 / math.sqrt(head_width)
    query_rows = (jnp.dot(hidden, w_qkv[0], preferred_element_type=jnp.float32) * inv_sqrt).astype(jnp.bfloat16)
    key_rows = jnp.dot(hidden, w_qkv[1], preferred_element_type=jnp.float32).astype(jnp.bfloat16)
    value_rows = jnp.dot(hidden, w_qkv[2], preferred_element_type=jnp.float32).astype(jnp.bfloat16)
    query_heads = query_rows.reshape(slot_count, HEADS, head_width).astype(jnp.float32)
    key_heads = key_rows.reshape(slot_count, HEADS, head_width).astype(jnp.float32)
    value_heads = value_rows.reshape(slot_count, HEADS, head_width).astype(jnp.float32)
    scores = jnp.einsum('qhe,khe->hqk', query_heads, key_heads)
    exp_scores = jnp.where(valid_keys[None, None, :], jnp.exp(scores), 0.0)
    attention = (exp_scores / lax.optimization_barrier(jnp.sum(exp_scores, axis=-1, keepdims=True))).astype(jnp.bfloat16)
    context = jnp.einsum('hqk,khe->qhe', attention.astype(jnp.float32), value_heads)
    context = context.astype(jnp.bfloat16).reshape(slot_count, D)
    mixed = norm_rows(hidden.astype(jnp.float32) + group_sum(context, w_out), gain_attn).astype(jnp.bfloat16)
    upward = jnp.dot(mixed, w_up, preferred_element_type=jnp.float32)
    activated = jax.nn.gelu(upward, approximate=False).astype(jnp.bfloat16)
    return norm_rows(mixed.astype(jnp.float32) + group_sum(activated, w_down), gain_mlp).astype(jnp.bfloat16)

def reference(query_states, doc_states, query_len, doc_len, doc_order, w_qkv, w_out, w_up, w_down, gain_attn, gain_mlp):

    def embed_sequence(item):
        states, seq_length = item
        positions = jnp.arange(states.shape[0], dtype=jnp.int32)
        valid_keys = positions < seq_length
        hidden = states
        for layer_index in range(w_qkv.shape[0]):
            hidden = encode_layer(hidden, valid_keys, w_qkv[layer_index], w_out[layer_index], w_up[layer_index], w_down[layer_index], gain_attn[layer_index], gain_mlp[layer_index])
        summed = lax.optimization_barrier(jnp.sum(jnp.where(valid_keys[:, None], hidden.astype(jnp.float32), 0.0), axis=0))
        pooled = summed / seq_length.astype(jnp.float32)
        return (pooled * lax.rsqrt(jnp.sum(pooled * pooled) + EPSILON)).astype(jnp.bfloat16)
    query_vectors = lax.map(embed_sequence, (query_states, query_len))
    document_vectors = lax.map(embed_sequence, (doc_states, doc_len))
    complete_scores = jnp.dot(query_vectors, document_vectors.T, preferred_element_type=jnp.float32) / SOFTMAX_TEMPER
    exp_total = lax.optimization_barrier(jnp.sum(jnp.exp(complete_scores), axis=1))
    shard_base = jnp.arange(N_DP, dtype=jnp.int32)[:, None] * PAIRS_DEV
    positive_index = (shard_base + doc_order.astype(jnp.int32)).reshape(-1)
    positive_score = jnp.take_along_axis(complete_scores, positive_index[:, None], axis=1)[:, 0]
    pair_loss = jnp.log(exp_total) - positive_score
    return (query_vectors, document_vectors, pair_loss)
```

```python
import functools
import math

import jax
import jax.numpy as jnp
from jax import lax
from jax.experimental import pallas as pl
from jax.experimental.pallas import tpu as pltpu
from jax.sharding import PartitionSpec as P

HEAD_WIDTH = 64
LANES = 128
CHUNK = 512
SOFTMAX_TEMPER = 0.05
EPSILON = 1e-06
LAYER_EPSILON = 1e-12


def norm_rows(values_in, gain_row):
    row_mean = jnp.mean(values_in, axis=-1, keepdims=True)
    centered = values_in - row_mean
    variance = jnp.mean(centered * centered, axis=-1, keepdims=True)
    return centered * lax.rsqrt(variance + LAYER_EPSILON) * gain_row


def gelu(x):
    return 0.5 * x * (1.0 + lax.erf(x * math.sqrt(0.5)))


def attention_kernel(shares, source_count, scalars, *refs):
    query_ref, doc_ref = refs[:2]
    passed_refs = refs[2 : 2 + source_count]
    weight_refs = refs[2 + source_count : -7]
    gain_ref, out_ref, hidden, w_in, w_ctx, total, sems = refs[-7:]
    groups = w_in.shape[0]
    width = w_ctx.shape[1]
    pairs_here = query_ref.shape[0]
    slot_count = hidden.shape[0]

    @pl.when(scalars[0] == 1)
    def _():
        source = scalars[2]
        entry = scalars[3]
        hidden_sem = sems.at[2 * groups]

        @pl.when((source == 0) & (entry < pairs_here))
        def _():
            pltpu.make_async_copy(
                query_ref.at[jnp.minimum(entry, pairs_here - 1)], hidden, hidden_sem
            ).start()

        @pl.when((source == 0) & (entry >= pairs_here))
        def _():
            pltpu.make_async_copy(
                doc_ref.at[jnp.clip(entry - pairs_here, 0, pairs_here - 1)], hidden, hidden_sem
            ).start()

        for number, (tag, ref) in enumerate(zip((1, 2), passed_refs)):

            @pl.when(source == tag)
            def _(ref=ref):
                pltpu.make_async_copy(ref, hidden, hidden_sem).start()

        first_copies, second_copies = [], []
        for group, members in enumerate(shares):
            first, second, offset = [], [], 0
            for member in members:
                qkv_ref, ctx_ref = weight_refs[2 * member], weight_refs[2 * member + 1]
                part = ctx_ref.shape[0]
                for kind in range(3):
                    first.append(
                        pltpu.make_async_copy(
                            qkv_ref.at[kind],
                            w_in.at[group, :, pl.ds(kind * width + offset, part)],
                            sems.at[group],
                        )
                    )
                second.append(
                    pltpu.make_async_copy(
                        ctx_ref, w_ctx.at[group, pl.ds(offset, part), :], sems.at[groups + group]
                    )
                )
                offset += part
            for copy in first + second:
                copy.start()
            first_copies.append(first)
            second_copies.append(second)

        pltpu.make_async_copy(query_ref.at[0], hidden, hidden_sem).wait()
        valid = lax.broadcasted_iota(jnp.int32, (1, slot_count), 1) < scalars[1]
        low_lanes = lax.broadcasted_iota(jnp.int32, (1, LANES), 1) < HEAD_WIDTH
        for group in range(groups):
            for copy in first_copies[group]:
                copy.wait()
            rows = jnp.dot(hidden[...], w_in[group], preferred_element_type=jnp.float32)
            queries = (rows[:, :width] * (1.0 / math.sqrt(HEAD_WIDTH))).astype(jnp.bfloat16)
            keys = rows[:, width : 2 * width].astype(jnp.bfloat16)
            values = rows[:, 2 * width :].astype(jnp.bfloat16)
            contexts = []
            for start in range(0, width, LANES):
                q2, k2, v2 = (a[:, start : start + LANES] for a in (queries, keys, values))
                halves = []
                for keep in (low_lanes, ~low_lanes):
                    q1 = jnp.where(keep, q2, jnp.zeros_like(q2))
                    scores = lax.dot_general(
                        q1, k2, (((1,), (1,)), ((), ())), preferred_element_type=jnp.float32
                    )
                    exps = jnp.where(valid, jnp.exp(scores), 0.0)
                    share = 1.0 / jnp.sum(exps, axis=-1, keepdims=True)
                    attention = (exps * share).astype(jnp.bfloat16)
                    halves.append(jnp.dot(attention, v2, preferred_element_type=jnp.float32))
                contexts.append(jnp.where(low_lanes, halves[0], halves[1]).astype(jnp.bfloat16))
            context = jnp.concatenate(contexts, axis=1)
            for copy in second_copies[group]:
                copy.wait()
            product = jnp.dot(context, w_ctx[group], preferred_element_type=jnp.float32)
            if group == 0:
                total[...] = hidden[...].astype(jnp.float32) + product
            else:
                total[...] += product
        out_ref[...] = norm_rows(total[...], gain_ref[...]).astype(jnp.bfloat16)


def attention_half(scalars, queries, docs, passed, weights, shares, gain):
    _, slot_count, model_width = queries.shape
    groups = len(shares)
    width = sum(weights[2 * member + 1].shape[0] for member in shares[0])
    far = pl.BlockSpec(memory_space=pltpu.HBM)
    near = pl.BlockSpec(memory_space=pltpu.VMEM)
    return pl.pallas_call(
        functools.partial(attention_kernel, shares, len(passed)),
        out_shape=jax.ShapeDtypeStruct((slot_count, model_width), jnp.bfloat16),
        in_specs=[pl.BlockSpec(memory_space=pltpu.SMEM)]
        + [far] * (2 + len(passed) + len(weights))
        + [near],
        out_specs=near,
        scratch_shapes=[
            pltpu.VMEM((slot_count, model_width), jnp.bfloat16),
            pltpu.VMEM((groups, model_width, 3 * width), jnp.bfloat16),
            pltpu.VMEM((groups, width, model_width), jnp.bfloat16),
            pltpu.VMEM((slot_count, model_width), jnp.float32),
            pltpu.SemaphoreType.DMA((2 * groups + 1,)),
        ],
        compiler_params=pltpu.CompilerParams(vmem_limit_bytes=40 * 2**20),
        name="attention_half",
    )(scalars, queries, docs, *passed, *weights, gain)


def mlp_kernel(scalars, hidden, *refs):
    weight_refs = refs[:-9]
    gain_ref, out_ref, pool_ref, w_up, w_down, before, total, sems, _ = refs[-9:]
    chunks = w_up.shape[0]
    chunk_width = w_up.shape[2]

    @pl.when(scalars[0] == 1)
    def _():
        copies = []
        for member in range(len(weight_refs) // 2):
            up_ref, down_ref = weight_refs[2 * member], weight_refs[2 * member + 1]
            for start in range(0, down_ref.shape[0], chunk_width):
                index = len(copies)
                copies.append(
                    (
                        pltpu.make_async_copy(
                            up_ref.at[:, pl.ds(start, chunk_width)],
                            w_up.at[index],
                            sems.at[index],
                        ),
                        pltpu.make_async_copy(
                            down_ref.at[pl.ds(start, chunk_width), :],
                            w_down.at[index],
                            sems.at[chunks + index],
                        ),
                    )
                )
                for copy in copies[-1]:
                    copy.start()
        copies[0][0].wait()
        before[0] = jnp.dot(hidden[...], w_up[0], preferred_element_type=jnp.float32)
        for index in range(chunks):
            if index + 1 < chunks:
                copies[index + 1][0].wait()
                before[(index + 1) % 2] = jnp.dot(
                    hidden[...], w_up[index + 1], preferred_element_type=jnp.float32
                )
            activated = gelu(before[index % 2]).astype(jnp.bfloat16)
            copies[index][1].wait()
            product = jnp.dot(activated, w_down[index], preferred_element_type=jnp.float32)
            if index == 0:
                total[...] = hidden[...].astype(jnp.float32) + product
            else:
                total[...] += product
        result = norm_rows(total[...], gain_ref[...]).astype(jnp.bfloat16)
        out_ref[...] = result
        used = lax.broadcasted_iota(jnp.int32, (result.shape[0], 1), 0) < scalars[1]
        pool_ref[...] = jnp.sum(
            jnp.where(used, result.astype(jnp.float32), 0.0), axis=0, keepdims=True
        )


def mlp_half(scalars, hidden, weights, gain):
    slot_count, model_width = hidden.shape
    hidden_units = sum(down.shape[0] for down in weights[1::2])
    chunks = hidden_units // CHUNK
    far = pl.BlockSpec(memory_space=pltpu.HBM)
    near = pl.BlockSpec(memory_space=pltpu.VMEM)
    return pl.pallas_call(
        mlp_kernel,
        out_shape=(
            jax.ShapeDtypeStruct((slot_count, model_width), jnp.bfloat16),
            jax.ShapeDtypeStruct((1, model_width), jnp.float32),
        ),
        in_specs=[pl.BlockSpec(memory_space=pltpu.SMEM), near] + [far] * len(weights) + [near],
        out_specs=(near, near),
        scratch_shapes=[
            pltpu.VMEM((chunks, model_width, CHUNK), jnp.bfloat16),
            pltpu.VMEM((chunks, CHUNK, model_width), jnp.bfloat16),
            pltpu.VMEM((2, slot_count, CHUNK), jnp.float32),
            pltpu.VMEM((slot_count, model_width), jnp.float32),
            pltpu.SemaphoreType.DMA((2 * chunks,)),
            pltpu.SMEM((1,), jnp.int32),
        ],
        compiler_params=pltpu.CompilerParams(vmem_limit_bytes=48 * 2**20),
        name="mlp_half",
    )(scalars, hidden, *weights, gain)


def half_of(piece, dim, which):
    size = piece.shape[dim] // 2
    return lax.dynamic_slice_in_dim(piece, which * size, size, dim)


def per_device(
    query_states,
    doc_states,
    query_len,
    doc_len,
    doc_order,
    w_qkv,
    w_out,
    w_up,
    w_down,
    gain_attn,
    gain_mlp,
):
    pair_count, slot_count, model_width = query_states.shape
    seq_count = 2 * pair_count
    dp_count = lax.axis_size("dp")
    dp_index = lax.axis_index("dp")
    section_count = lax.axis_size("pipe")
    section = lax.axis_index("pipe")
    tensor_count = lax.axis_size("tensor")
    tensor_index = lax.axis_index("tensor")
    side = tensor_count // 2
    batch = seq_count // 2

    own = [w_qkv[0], w_out[0], w_up[0], w_down[0]]
    half_dims = (2, 0, 1, 0)
    shards = [own]
    for step in range(1, side):
        to_middle = [(side - 1 - step, side - 1), (side + step, side)]
        shards.append([lax.ppermute(piece, "tensor", to_middle) for piece in own])
    across = [(side - 1, side), (side, side - 1)]
    swap = [(index, index ^ 1) for index in range(dp_count)]
    pieces = list(shards)
    groups = [(index,) for index in range(side)]
    for shard in shards:
        if dp_count % 2 == 0:
            sent = [half_of(piece, dim, dp_index % 2) for piece, dim in zip(shard, half_dims)]
            near_half = [lax.ppermute(piece, "tensor", across) for piece in sent]
            far_half = [lax.ppermute(piece, "dp", swap) for piece in near_half]
            groups.append((len(pieces), len(pieces) + 1))
            pieces += [near_half, far_half]
        else:
            groups.append((len(pieces),))
            pieces.append([lax.ppermute(piece, "tensor", across) for piece in shard])
    attention_weights = [array for piece in pieces for array in piece[:2]]
    mlp_weights = [array for piece in pieces for array in piece[2:]]

    lengths = jnp.concatenate([query_len, doc_len])
    host = jnp.clip(tensor_index - (side - 1), 0, 1)
    is_host = (tensor_index == side - 1) | (tensor_index == side)

    def lag(index):
        return index + index // 2

    slots = lag(section_count - 1) + batch
    outputs, fast, slow, sums = [], {}, {}, []
    for slot in range(slots):
        local = slot - lag(section)
        active = (local >= 0) & (local < batch) & is_host
        entry = host * batch + jnp.clip(local, 0, batch - 1)
        source = jnp.where(section == 0, 0, jnp.where(section % 2 == 1, 1, 2))
        scalars = jnp.stack(
            [active.astype(jnp.int32), lengths[entry], source.astype(jnp.int32), entry]
        ).astype(jnp.int32)
        passed = [
            fast.get(slot - 1, query_states[0]),
            slow.get(slot - 2, query_states[0]),
        ]
        mixed = attention_half(
            scalars, query_states, doc_states, passed, attention_weights, groups, gain_attn
        )
        hidden, pool = mlp_half(scalars, mixed, mlp_weights, gain_mlp)
        sums.append(pool)
        for step, table in ((0, fast), (1, slow)):
            moves = [
                (index, index + 1)
                for index in range(step, section_count - 1, 2)
                if 0 <= slot - lag(index) < batch
            ]
            if moves:
                table[slot] = lax.ppermute(hidden, "pipe", moves)

    summed = jnp.concatenate(sums[slots - batch :], axis=0)
    own_lengths = lax.dynamic_slice_in_dim(lengths, host * batch, batch, 0)
    pooled = summed / own_lengths.astype(jnp.float32)[:, None]
    embedded = (
        pooled * lax.rsqrt(jnp.sum(pooled * pooled, axis=1, keepdims=True) + EPSILON)
    ).astype(jnp.bfloat16)
    places = dp_count * 2
    own_place = (lax.broadcasted_iota(jnp.int32, (places, 1, 1), 0) == dp_index * 2 + host) & (
        is_host & (section == section_count - 1)
    )
    table = jnp.where(own_place, embedded[None], jnp.zeros_like(embedded)[None])
    table = lax.psum(table, ("dp", "pipe", "tensor")).astype(jnp.bfloat16)
    table = table.reshape(dp_count, seq_count, model_width)
    mine = lax.dynamic_index_in_dim(table, dp_index, 0, keepdims=False)
    local_queries, local_docs = mine[:pair_count], mine[pair_count:]
    all_docs = table[:, pair_count:].reshape(dp_count * pair_count, model_width)
    scores = (
        lax.dot_general(
            local_queries,
            all_docs,
            (((1,), (1,)), ((), ())),
            preferred_element_type=jnp.float32,
        )
        / SOFTMAX_TEMPER
    )
    columns = jnp.arange(dp_count * pair_count, dtype=jnp.int32)
    positive = dp_index * pair_count + doc_order[0]
    positive_score = jnp.sum(
        jnp.where(columns[None, :] == positive[:, None], scores, 0.0), axis=1
    )
    pair_loss = jnp.log(jnp.sum(jnp.exp(scores), axis=1)) - positive_score
    piece_width = model_width // (section_count * tensor_count)
    first = (section * tensor_count + tensor_index) * piece_width
    return (
        lax.dynamic_slice_in_dim(local_queries, first, piece_width, 1),
        lax.dynamic_slice_in_dim(local_docs, first, piece_width, 1),
        pair_loss,
    )


def solution(mesh):
    in_specs = (
        P("dp", None, None),
        P("dp", None, None),
        P("dp"),
        P("dp"),
        P("dp", None),
        P("pipe", None, None, "tensor"),
        P("pipe", "tensor", None),
        P("pipe", None, "tensor"),
        P("pipe", "tensor", None),
        P("pipe", None),
        P("pipe", None),
    )
    out_specs = (P("dp", ("pipe", "tensor")), P("dp", ("pipe", "tensor")), P("dp"))
    return jax.shard_map(
        per_device, mesh=mesh, in_specs=in_specs, out_specs=out_specs, check_vma=False
    )
```

```python
import functools
import math

import jax
import jax.numpy as jnp
from jax import lax
from jax.experimental import pallas as pl
from jax.experimental.pallas import tpu as pltpu
from jax.sharding import PartitionSpec as P

HEAD_WIDTH = 64
LANES = 128
SOFTMAX_TEMPER = 0.05
EPSILON = 1e-06
LAYER_EPSILON = 1e-12


def norm_rows(values_in, gain_row):
    row_mean = jnp.mean(values_in, axis=-1, keepdims=True)
    centered = values_in - row_mean
    variance = jnp.mean(centered * centered, axis=-1, keepdims=True)
    return centered * lax.rsqrt(variance + LAYER_EPSILON) * gain_row


def gelu(x):
    return 0.5 * x * (1.0 + lax.erf(x * math.sqrt(0.5)))


def start_attention_weights(group, refs, w_in, w_ctx, sems):
    groups = w_in.shape[0]
    width = w_ctx.shape[1]
    offset = 0
    if len(refs) == 2 and refs[0].shape[0] == 3:
        members = [(refs[0], lambda column: refs[1].at[:, column], width)]
    else:
        members = [
            (ref, lambda column, ref=ref: ref.at[3, column, :], ref.shape[2]) for ref in refs
        ]
    for qkv, ctx_block, part in members:
        for kind in range(3):
            pltpu.make_async_copy(
                qkv.at[kind],
                w_in.at[group, :, pl.ds(kind * width + offset, part)],
                sems.at[group],
            ).start()
        for start in range(0, w_ctx.shape[2], part):
            pltpu.make_async_copy(
                ctx_block(pl.ds(start, part)),
                w_ctx.at[group, pl.ds(offset, part), pl.ds(start, part)],
                sems.at[groups + group],
            ).start()
        offset += part


def attention_kernel(slot, shares, source_count, plan, *refs):
    query_ref, doc_ref = refs[:2]
    passed_refs = refs[2 : 2 + source_count]
    weight_refs = refs[2 + source_count : -7]
    gain_ref, out_ref, hidden, w_in, w_ctx, total, sems = refs[-7:]
    groups = w_in.shape[0]
    width = w_ctx.shape[1]
    pairs_here = query_ref.shape[0]
    slot_count = hidden.shape[0]

    @pl.when(plan[slot, 0] == 1)
    def _():
        source = plan[slot, 2]
        entry = plan[slot, 3]
        hidden_sem = sems.at[2 * groups]

        @pl.when((source == 0) & (entry < pairs_here))
        def _():
            pltpu.make_async_copy(
                query_ref.at[jnp.minimum(entry, pairs_here - 1)], hidden, hidden_sem
            ).start()

        @pl.when((source == 0) & (entry >= pairs_here))
        def _():
            pltpu.make_async_copy(
                doc_ref.at[jnp.clip(entry - pairs_here, 0, pairs_here - 1)], hidden, hidden_sem
            ).start()

        for tag, ref in zip((1, 2), passed_refs):

            @pl.when(source == tag)
            def _(ref=ref):
                pltpu.make_async_copy(ref, hidden, hidden_sem).start()

        for group, members in enumerate(shares):
            start_attention_weights(
                group, [weight_refs[member] for member in members], w_in, w_ctx, sems
            )
        pltpu.make_async_copy(query_ref.at[0], hidden, hidden_sem).wait()
        valid = lax.broadcasted_iota(jnp.int32, (1, slot_count), 1) < plan[slot, 1]
        low_lanes = lax.broadcasted_iota(jnp.int32, (1, LANES), 1) < HEAD_WIDTH
        total[...] = hidden[...].astype(jnp.float32)

        def one_group(group, carry):
            pltpu.make_async_copy(w_in.at[group], w_in.at[group], sems.at[group]).wait()
            pltpu.make_async_copy(w_ctx.at[group], w_ctx.at[group], sems.at[groups + group]).wait()
            rows = jnp.dot(hidden[...], w_in[group], preferred_element_type=jnp.float32)
            queries = (rows[:, :width] * (1.0 / math.sqrt(HEAD_WIDTH))).astype(jnp.bfloat16)
            keys = rows[:, width : 2 * width].astype(jnp.bfloat16)
            values = rows[:, 2 * width :].astype(jnp.bfloat16)
            contexts = []
            for start in range(0, width, LANES):
                q2, k2, v2 = (a[:, start : start + LANES] for a in (queries, keys, values))
                halves = []
                for keep in (low_lanes, ~low_lanes):
                    q1 = jnp.where(keep, q2, jnp.zeros_like(q2))
                    scores = lax.dot_general(
                        q1, k2, (((1,), (1,)), ((), ())), preferred_element_type=jnp.float32
                    )
                    exps = jnp.where(valid, jnp.exp(scores), 0.0)
                    share = 1.0 / jnp.sum(exps, axis=-1, keepdims=True)
                    attention = (exps * share).astype(jnp.bfloat16)
                    halves.append(jnp.dot(attention, v2, preferred_element_type=jnp.float32))
                contexts.append(jnp.where(low_lanes, halves[0], halves[1]).astype(jnp.bfloat16))
            context = jnp.concatenate(contexts, axis=1)
            total[...] += jnp.dot(context, w_ctx[group], preferred_element_type=jnp.float32)
            return carry

        lax.fori_loop(0, groups, one_group, 0)
        out_ref[...] = norm_rows(total[...], gain_ref[...]).astype(jnp.bfloat16)


def attention_half(slot, plan, queries, docs, passed, weights, shares, gain):
    _, slot_count, model_width = queries.shape
    groups = len(shares)
    width = weights[1].shape[0]
    far = pl.BlockSpec(memory_space=pltpu.HBM)
    near = pl.BlockSpec(memory_space=pltpu.VMEM)
    return pl.pallas_call(
        functools.partial(attention_kernel, slot, shares, len(passed)),
        out_shape=jax.ShapeDtypeStruct((slot_count, model_width), jnp.bfloat16),
        in_specs=[pl.BlockSpec(memory_space=pltpu.SMEM)]
        + [far] * (2 + len(passed) + len(weights))
        + [near],
        out_specs=near,
        scratch_shapes=[
            pltpu.VMEM((slot_count, model_width), jnp.bfloat16),
            pltpu.VMEM((groups, model_width, 3 * width), jnp.bfloat16),
            pltpu.VMEM((groups, width, model_width), jnp.bfloat16),
            pltpu.VMEM((slot_count, model_width), jnp.float32),
            pltpu.SemaphoreType.DMA((2 * groups + 1,)),
        ],
        compiler_params=pltpu.CompilerParams(vmem_limit_bytes=40 * 2**20),
        name="attention_half",
    )(plan, queries, docs, *passed, *weights, gain)


def mlp_kernel(slot, plan, hidden, *refs):
    weight_refs = refs[:-7]
    gain_ref, out_ref, pool_ref, w_up, w_down, total, sems = refs[-7:]
    chunks = w_up.shape[0]
    chunk_width = w_up.shape[2]

    @pl.when(plan[slot, 0] == 1)
    def _():
        index = 0
        for member in range(len(weight_refs) // 2):
            up_ref, down_ref = weight_refs[2 * member], weight_refs[2 * member + 1]
            for start in range(0, down_ref.shape[0], chunk_width):
                pltpu.make_async_copy(
                    up_ref.at[:, pl.ds(start, chunk_width)], w_up.at[index], sems.at[index]
                ).start()
                pltpu.make_async_copy(
                    down_ref.at[pl.ds(start, chunk_width), :],
                    w_down.at[index],
                    sems.at[chunks + index],
                ).start()
                index += 1
        total[...] = hidden[...].astype(jnp.float32)

        def one_chunk(chunk, carry):
            pltpu.make_async_copy(w_up.at[chunk], w_up.at[chunk], sems.at[chunk]).wait()
            pltpu.make_async_copy(w_down.at[chunk], w_down.at[chunk], sems.at[chunks + chunk]).wait()
            before = jnp.dot(hidden[...], w_up[chunk], preferred_element_type=jnp.float32)
            total[...] += jnp.dot(
                gelu(before).astype(jnp.bfloat16),
                w_down[chunk],
                preferred_element_type=jnp.float32,
            )
            return carry

        lax.fori_loop(0, chunks, one_chunk, 0)
        result = norm_rows(total[...], gain_ref[...]).astype(jnp.bfloat16)
        out_ref[...] = result
        used = lax.broadcasted_iota(jnp.int32, (result.shape[0], 1), 0) < plan[slot, 1]
        pool_ref[...] = jnp.sum(
            jnp.where(used, result.astype(jnp.float32), 0.0), axis=0, keepdims=True
        )


def mlp_half(slot, plan, hidden, weights, gain):
    slot_count, model_width = hidden.shape
    chunk_width = min(down.shape[0] for down in weights[1::2])
    chunks = sum(down.shape[0] for down in weights[1::2]) // chunk_width
    far = pl.BlockSpec(memory_space=pltpu.HBM)
    near = pl.BlockSpec(memory_space=pltpu.VMEM)
    return pl.pallas_call(
        functools.partial(mlp_kernel, slot),
        out_shape=(
            jax.ShapeDtypeStruct((slot_count, model_width), jnp.bfloat16),
            jax.ShapeDtypeStruct((1, model_width), jnp.float32),
        ),
        in_specs=[pl.BlockSpec(memory_space=pltpu.SMEM), near] + [far] * len(weights) + [near],
        out_specs=(near, near),
        scratch_shapes=[
            pltpu.VMEM((chunks, model_width, chunk_width), jnp.bfloat16),
            pltpu.VMEM((chunks, chunk_width, model_width), jnp.bfloat16),
            pltpu.VMEM((slot_count, model_width), jnp.float32),
            pltpu.SemaphoreType.DMA((2 * chunks,)),
        ],
        compiler_params=pltpu.CompilerParams(vmem_limit_bytes=48 * 2**20),
        name="mlp_half",
    )(plan, hidden, *weights, gain)


def half_shard(w_qkv, w_out, w_up, w_down, which):
    def cut(piece, dim):
        size = piece.shape[dim] // 2
        return lax.dynamic_slice_in_dim(piece, which * size, size, dim)

    qkv, out = cut(w_qkv, 2), cut(w_out, 0)
    part, width = out.shape
    blocks = out.reshape(part, width // part, part).swapaxes(0, 1).reshape(1, width, part)
    return [jnp.concatenate([qkv, blocks], axis=0), cut(w_up, 1), cut(w_down, 0)]


def per_device(
    query_states,
    doc_states,
    query_len,
    doc_len,
    doc_order,
    w_qkv,
    w_out,
    w_up,
    w_down,
    gain_attn,
    gain_mlp,
):
    pair_count, _, model_width = query_states.shape
    seq_count = 2 * pair_count
    dp_count = lax.axis_size("dp")
    dp_index = lax.axis_index("dp")
    section_count = lax.axis_size("pipe")
    section = lax.axis_index("pipe")
    tensor_count = lax.axis_size("tensor")
    tensor_index = lax.axis_index("tensor")
    side = tensor_count // 2
    batch = seq_count // 2

    shared = dp_count % 2 == 0
    parity = dp_index % 2 if shared else 0
    mine = (w_qkv[0], w_out[0], w_up[0], w_down[0])
    own_first, own_second = (half_shard(*mine, which) for which in (parity, 1 - parity))
    across = [(side - 1, side), (side, side - 1)]
    swap = [(index, index ^ 1) for index in range(dp_count)]

    inwards = [[(side - 1 - step, side - 1), (side + step, side)] for step in range(1, side)]
    kinds = len(own_first)
    firsts = [own_first] + [[] for _ in inwards]
    seconds = [own_second] + [[] for _ in inwards]
    crossed = [[] for _ in firsts]
    swapped = [[] for _ in firsts]
    for kind in range(kinds):
        for index, pairs in enumerate(inwards):
            firsts[index + 1].append(lax.ppermute(own_first[kind], "tensor", pairs))
        crossed[0].append(lax.ppermute(own_first[kind], "tensor", across))
    for kind in range(kinds):
        for index, pairs in enumerate(inwards):
            seconds[index + 1].append(lax.ppermute(own_second[kind], "tensor", pairs))

    def pass_on(index, kind):
        if shared:
            swapped[index].append(lax.ppermute(crossed[index][kind], "dp", swap))
        else:
            swapped[index].append(lax.ppermute(seconds[index][kind], "tensor", across))

    for kind in range(kinds):
        for index in range(1, side):
            crossed[index].append(lax.ppermute(firsts[index][kind], "tensor", across))
        pass_on(0, kind)
        if kind > 0:
            for index in range(1, side):
                pass_on(index, kind - 1)
    for index in range(1, side):
        pass_on(index, kinds - 1)
    halves = []
    for index in range(1, side):
        halves += [firsts[index], seconds[index]]
    for index in range(side):
        halves += [crossed[index], swapped[index]]
    attention_weights = [mine[0], mine[1]] + [half[0] for half in halves]
    groups = [(0, 1)] + [(2 + i, 3 + i) for i in range(0, len(halves), 2)]
    mlp_weights = [mine[2], mine[3]] + [piece for half in halves for piece in half[1:]]

    lengths = jnp.concatenate([query_len, doc_len])
    host = jnp.clip(tensor_index - (side - 1), 0, 1)
    is_host = (tensor_index == side - 1) | (tensor_index == side)

    def lag(index):
        return index + index // 2

    slots = lag(section_count - 1) + batch
    steps = jnp.arange(slots, dtype=jnp.int32)
    local = steps - lag(section)
    active = (local >= 0) & (local < batch) & is_host
    entry = host * batch + jnp.clip(local, 0, batch - 1)
    picks = entry[:, None] == jnp.arange(seq_count, dtype=jnp.int32)[None, :]
    slot_lengths = jnp.sum(jnp.where(picks, lengths[None, :], 0), axis=1)
    source = jnp.where(section == 0, 0, jnp.where(section % 2 == 1, 1, 2))
    plan = jnp.stack(
        [active.astype(jnp.int32), slot_lengths, jnp.full_like(steps, source), entry], axis=1
    ).astype(jnp.int32)
    fast, slow, sums = {}, {}, []
    for slot in range(slots):
        passed = [
            fast.get(slot - 1, query_states[0]),
            slow.get(slot - 2, query_states[0]),
        ]
        mixed = attention_half(
            slot, plan, query_states, doc_states, passed, attention_weights, groups, gain_attn
        )
        hidden, pool = mlp_half(slot, plan, mixed, mlp_weights, gain_mlp)
        sums.append(pool)
        for step, table in ((0, fast), (1, slow)):
            moves = [
                (index, index + 1)
                for index in range(step, section_count - 1, 2)
                if 0 <= slot - lag(index) < batch
            ]
            if moves:
                table[slot] = lax.ppermute(hidden, "pipe", moves)

    summed = jnp.concatenate(sums[slots - batch :], axis=0)
    own_lengths = lax.dynamic_slice_in_dim(lengths, host * batch, batch, 0)
    pooled = summed / own_lengths.astype(jnp.float32)[:, None]
    embedded = (
        pooled * lax.rsqrt(jnp.sum(pooled * pooled, axis=1, keepdims=True) + EPSILON)
    ).astype(jnp.bfloat16)
    embedded = jnp.where(is_host & (section == section_count - 1), embedded, jnp.zeros_like(embedded))
    table = lax.psum(lax.all_gather(embedded, "dp"), "pipe")
    table = jnp.where(
        jnp.arange(2, dtype=jnp.int32)[None, :, None, None] == host,
        table[:, None],
        jnp.zeros_like(table)[:, None],
    )
    table = lax.psum(table, "tensor").astype(jnp.bfloat16)
    table = table.reshape(dp_count, seq_count, model_width)
    mine = lax.dynamic_index_in_dim(table, dp_index, 0, keepdims=False)
    local_queries, local_docs = mine[:pair_count], mine[pair_count:]
    all_docs = table[:, pair_count:].reshape(dp_count * pair_count, model_width)
    scores = (
        lax.dot_general(
            local_queries,
            all_docs,
            (((1,), (1,)), ((), ())),
            preferred_element_type=jnp.float32,
        )
        / SOFTMAX_TEMPER
    )
    columns = jnp.arange(dp_count * pair_count, dtype=jnp.int32)
    positive = dp_index * pair_count + doc_order[0]
    positive_score = jnp.sum(
        jnp.where(columns[None, :] == positive[:, None], scores, 0.0), axis=1
    )
    pair_loss = jnp.log(jnp.sum(jnp.exp(scores), axis=1)) - positive_score
    piece_width = model_width // (section_count * tensor_count)
    first = (section * tensor_count + tensor_index) * piece_width
    return (
        lax.dynamic_slice_in_dim(local_queries, first, piece_width, 1),
        lax.dynamic_slice_in_dim(local_docs, first, piece_width, 1),
        pair_loss,
    )


def solution(mesh):
    in_specs = (
        P("dp", None, None),
        P("dp", None, None),
        P("dp"),
        P("dp"),
        P("dp", None),
        P("pipe", None, None, "tensor"),
        P("pipe", "tensor", None),
        P("pipe", None, "tensor"),
        P("pipe", "tensor", None),
        P("pipe", None),
        P("pipe", None),
    )
    out_specs = (P("dp", ("pipe", "tensor")), P("dp", ("pipe", "tensor")), P("dp"))
    return jax.shard_map(
        per_device, mesh=mesh, in_specs=in_specs, out_specs=out_specs, check_vma=False
    )
```

```python
import functools
import math

import jax
import jax.numpy as jnp
from jax import lax
from jax.experimental import pallas as pl
from jax.experimental.pallas import tpu as pltpu
from jax.sharding import PartitionSpec as P

HEAD_WIDTH = 64
LANES = 128
SOFTMAX_TEMPER = 0.05
EPSILON = 1e-06
LAYER_EPSILON = 1e-12


def norm_rows(values_in, gain_row):
    row_mean = jnp.mean(values_in, axis=-1, keepdims=True)
    centered = values_in - row_mean
    variance = jnp.mean(centered * centered, axis=-1, keepdims=True)
    return centered * lax.rsqrt(variance + LAYER_EPSILON) * gain_row


def gelu(x):
    return 0.5 * x * (1.0 + lax.erf(x * math.sqrt(0.5)))


def start_attention_weights(group, refs, w_in, w_ctx, sems):
    groups = w_in.shape[0]
    width = w_ctx.shape[1]
    offset = 0
    if len(refs) == 2 and refs[0].shape[0] == 3:
        members = [(refs[0], lambda column: refs[1].at[:, column], width)]
    else:
        members = [
            (ref, lambda column, ref=ref: ref.at[3, column, :], ref.shape[2]) for ref in refs
        ]
    for qkv, ctx_block, part in members:
        for kind in range(3):
            pltpu.make_async_copy(
                qkv.at[kind],
                w_in.at[group, :, pl.ds(kind * width + offset, part)],
                sems.at[group],
            ).start()
        for start in range(0, w_ctx.shape[2], part):
            pltpu.make_async_copy(
                ctx_block(pl.ds(start, part)),
                w_ctx.at[group, pl.ds(offset, part), pl.ds(start, part)],
                sems.at[groups + group],
            ).start()
        offset += part


def attention_kernel(slot, shares, source_count, plan, *refs):
    query_ref, doc_ref = refs[:2]
    passed_refs = refs[2 : 2 + source_count]
    weight_refs = refs[2 + source_count : -7]
    gain_ref, out_ref, hidden, w_in, w_ctx, total, sems = refs[-7:]
    groups = w_in.shape[0]
    width = w_ctx.shape[1]
    pairs_here = query_ref.shape[0]
    slot_count = hidden.shape[0]

    @pl.when(plan[slot, 0] == 1)
    def _():
        source = plan[slot, 2]
        entry = plan[slot, 3]
        hidden_sem = sems.at[2 * groups]

        @pl.when((source == 0) & (entry < pairs_here))
        def _():
            pltpu.make_async_copy(
                query_ref.at[jnp.minimum(entry, pairs_here - 1)], hidden, hidden_sem
            ).start()

        @pl.when((source == 0) & (entry >= pairs_here))
        def _():
            pltpu.make_async_copy(
                doc_ref.at[jnp.clip(entry - pairs_here, 0, pairs_here - 1)], hidden, hidden_sem
            ).start()

        for tag, ref in zip((1, 2), passed_refs):

            @pl.when(source == tag)
            def _(ref=ref):
                pltpu.make_async_copy(ref, hidden, hidden_sem).start()

        for group, members in enumerate(shares):
            start_attention_weights(
                group, [weight_refs[member] for member in members], w_in, w_ctx, sems
            )
        pltpu.make_async_copy(query_ref.at[0], hidden, hidden_sem).wait()
        valid = lax.broadcasted_iota(jnp.int32, (1, slot_count), 1) < plan[slot, 1]
        low_lanes = lax.broadcasted_iota(jnp.int32, (1, LANES), 1) < HEAD_WIDTH
        total[...] = hidden[...].astype(jnp.float32)

        def one_group(group, carry):
            pltpu.make_async_copy(w_in.at[group], w_in.at[group], sems.at[group]).wait()
            pltpu.make_async_copy(w_ctx.at[group], w_ctx.at[group], sems.at[groups + group]).wait()
            rows = jnp.dot(hidden[...], w_in[group], preferred_element_type=jnp.float32)
            queries = (rows[:, :width] * (1.0 / math.sqrt(HEAD_WIDTH))).astype(jnp.bfloat16)
            keys = rows[:, width : 2 * width].astype(jnp.bfloat16)
            values = rows[:, 2 * width :].astype(jnp.bfloat16)
            contexts = []
            for start in range(0, width, LANES):
                q2, k2, v2 = (a[:, start : start + LANES] for a in (queries, keys, values))
                halves = []
                for keep in (low_lanes, ~low_lanes):
                    q1 = jnp.where(keep, q2, jnp.zeros_like(q2))
                    scores = lax.dot_general(
                        q1, k2, (((1,), (1,)), ((), ())), preferred_element_type=jnp.float32
                    )
                    exps = jnp.where(valid, jnp.exp(scores), 0.0)
                    share = 1.0 / jnp.sum(exps, axis=-1, keepdims=True)
                    attention = (exps * share).astype(jnp.bfloat16)
                    halves.append(jnp.dot(attention, v2, preferred_element_type=jnp.float32))
                contexts.append(jnp.where(low_lanes, halves[0], halves[1]).astype(jnp.bfloat16))
            context = jnp.concatenate(contexts, axis=1)
            total[...] += jnp.dot(context, w_ctx[group], preferred_element_type=jnp.float32)
            return carry

        lax.fori_loop(0, groups, one_group, 0)
        out_ref[...] = norm_rows(total[...], gain_ref[...]).astype(jnp.bfloat16)


def attention_half(slot, plan, queries, docs, passed, weights, shares, gain):
    _, slot_count, model_width = queries.shape
    groups = len(shares)
    width = weights[1].shape[0]
    far = pl.BlockSpec(memory_space=pltpu.HBM)
    near = pl.BlockSpec(memory_space=pltpu.VMEM)
    return pl.pallas_call(
        functools.partial(attention_kernel, slot, shares, len(passed)),
        out_shape=jax.ShapeDtypeStruct((slot_count, model_width), jnp.bfloat16),
        in_specs=[pl.BlockSpec(memory_space=pltpu.SMEM)]
        + [far] * (2 + len(passed) + len(weights))
        + [near],
        out_specs=near,
        scratch_shapes=[
            pltpu.VMEM((slot_count, model_width), jnp.bfloat16),
            pltpu.VMEM((groups, model_width, 3 * width), jnp.bfloat16),
            pltpu.VMEM((groups, width, model_width), jnp.bfloat16),
            pltpu.VMEM((slot_count, model_width), jnp.float32),
            pltpu.SemaphoreType.DMA((2 * groups + 1,)),
        ],
        compiler_params=pltpu.CompilerParams(vmem_limit_bytes=40 * 2**20),
        name="attention_half",
    )(plan, queries, docs, *passed, *weights, gain)


def mlp_kernel(slot, plan, hidden, *refs):
    weight_refs = refs[:-7]
    gain_ref, out_ref, pool_ref, w_up, w_down, total, sems = refs[-7:]
    chunks = w_up.shape[0]
    chunk_width = w_up.shape[2]

    @pl.when(plan[slot, 0] == 1)
    def _():
        index = 0
        for member in range(len(weight_refs) // 2):
            up_ref, down_ref = weight_refs[2 * member], weight_refs[2 * member + 1]
            for start in range(0, down_ref.shape[0], chunk_width):
                pltpu.make_async_copy(
                    up_ref.at[:, pl.ds(start, chunk_width)], w_up.at[index], sems.at[index]
                ).start()
                pltpu.make_async_copy(
                    down_ref.at[pl.ds(start, chunk_width), :],
                    w_down.at[index],
                    sems.at[chunks + index],
                ).start()
                index += 1
        total[...] = hidden[...].astype(jnp.float32)

        def one_chunk(chunk, carry):
            pltpu.make_async_copy(w_up.at[chunk], w_up.at[chunk], sems.at[chunk]).wait()
            pltpu.make_async_copy(w_down.at[chunk], w_down.at[chunk], sems.at[chunks + chunk]).wait()
            before = jnp.dot(hidden[...], w_up[chunk], preferred_element_type=jnp.float32)
            total[...] += jnp.dot(
                gelu(before).astype(jnp.bfloat16),
                w_down[chunk],
                preferred_element_type=jnp.float32,
            )
            return carry

        lax.fori_loop(0, chunks, one_chunk, 0)
        result = norm_rows(total[...], gain_ref[...]).astype(jnp.bfloat16)
        out_ref[...] = result
        used = lax.broadcasted_iota(jnp.int32, (result.shape[0], 1), 0) < plan[slot, 1]
        pool_ref[...] = jnp.sum(
            jnp.where(used, result.astype(jnp.float32), 0.0), axis=0, keepdims=True
        )


def mlp_half(slot, plan, hidden, weights, gain):
    slot_count, model_width = hidden.shape
    chunk_width = min(down.shape[0] for down in weights[1::2])
    chunks = sum(down.shape[0] for down in weights[1::2]) // chunk_width
    far = pl.BlockSpec(memory_space=pltpu.HBM)
    near = pl.BlockSpec(memory_space=pltpu.VMEM)
    return pl.pallas_call(
        functools.partial(mlp_kernel, slot),
        out_shape=(
            jax.ShapeDtypeStruct((slot_count, model_width), jnp.bfloat16),
            jax.ShapeDtypeStruct((1, model_width), jnp.float32),
        ),
        in_specs=[pl.BlockSpec(memory_space=pltpu.SMEM), near] + [far] * len(weights) + [near],
        out_specs=(near, near),
        scratch_shapes=[
            pltpu.VMEM((chunks, model_width, chunk_width), jnp.bfloat16),
            pltpu.VMEM((chunks, chunk_width, model_width), jnp.bfloat16),
            pltpu.VMEM((slot_count, model_width), jnp.float32),
            pltpu.SemaphoreType.DMA((2 * chunks,)),
        ],
        compiler_params=pltpu.CompilerParams(vmem_limit_bytes=48 * 2**20),
        name="mlp_half",
    )(plan, hidden, *weights, gain)


def half_shard(w_qkv, w_out, w_up, w_down, which):
    def cut(piece, dim):
        size = piece.shape[dim] // 2
        return lax.dynamic_slice_in_dim(piece, which * size, size, dim)

    qkv, out = cut(w_qkv, 2), cut(w_out, 0)
    part, width = out.shape
    blocks = out.reshape(part, width // part, part).swapaxes(0, 1).reshape(1, width, part)
    return [jnp.concatenate([qkv, blocks], axis=0), cut(w_up, 1), cut(w_down, 0)]


def per_device(
    query_states,
    doc_states,
    query_len,
    doc_len,
    doc_order,
    w_qkv,
    w_out,
    w_up,
    w_down,
    gain_attn,
    gain_mlp,
):
    pair_count, _, model_width = query_states.shape
    seq_count = 2 * pair_count
    dp_count = lax.axis_size("dp")
    dp_index = lax.axis_index("dp")
    section_count = lax.axis_size("pipe")
    section = lax.axis_index("pipe")
    tensor_count = lax.axis_size("tensor")
    tensor_index = lax.axis_index("tensor")
    side = tensor_count // 2
    batch = seq_count // 2

    shared = dp_count % 2 == 0
    parity = dp_index % 2 if shared else 0
    mine = (w_qkv[0], w_out[0], w_up[0], w_down[0])
    own_first, own_second = (half_shard(*mine, which) for which in (parity, 1 - parity))
    across = [(side - 1, side), (side, side - 1)]
    swap = [(index, index ^ 1) for index in range(dp_count)]

    inwards = [[(side - 1 - step, side - 1), (side + step, side)] for step in range(1, side)]
    kinds = len(own_first)
    firsts = [own_first] + [[] for _ in inwards]
    seconds = [own_second] + [[] for _ in inwards]
    crossed = [[] for _ in firsts]
    swapped = [[] for _ in firsts]
    for kind in range(kinds):
        for index, pairs in enumerate(inwards):
            firsts[index + 1].append(lax.ppermute(own_first[kind], "tensor", pairs))
        crossed[0].append(lax.ppermute(own_first[kind], "tensor", across))
    for kind in range(kinds):
        for index, pairs in enumerate(inwards):
            seconds[index + 1].append(lax.ppermute(own_second[kind], "tensor", pairs))

    def pass_on(index, kind):
        if shared:
            swapped[index].append(lax.ppermute(crossed[index][kind], "dp", swap))
        else:
            swapped[index].append(lax.ppermute(seconds[index][kind], "tensor", across))

    for kind in range(kinds):
        for index in range(1, side):
            crossed[index].append(lax.ppermute(firsts[index][kind], "tensor", across))
        pass_on(0, kind)
    for kind in range(kinds):
        for index in range(1, side):
            pass_on(index, kind)
    halves = []
    for index in range(1, side):
        halves += [firsts[index], seconds[index]]
    for index in range(side):
        halves += [crossed[index], swapped[index]]
    attention_weights = [mine[0], mine[1]] + [half[0] for half in halves]
    groups = [(0, 1)] + [(2 + i, 3 + i) for i in range(0, len(halves), 2)]
    mlp_weights = [mine[2], mine[3]] + [piece for half in halves for piece in half[1:]]

    lengths = jnp.concatenate([query_len, doc_len])
    host = jnp.clip(tensor_index - (side - 1), 0, 1)
    is_host = (tensor_index == side - 1) | (tensor_index == side)

    def lag(index):
        return index + index // 2

    slots = lag(section_count - 1) + batch
    steps = jnp.arange(slots, dtype=jnp.int32)
    local = steps - lag(section)
    active = (local >= 0) & (local < batch) & is_host
    entry = host * batch + jnp.clip(local, 0, batch - 1)
    picks = entry[:, None] == jnp.arange(seq_count, dtype=jnp.int32)[None, :]
    slot_lengths = jnp.sum(jnp.where(picks, lengths[None, :], 0), axis=1)
    source = jnp.where(section == 0, 0, jnp.where(section % 2 == 1, 1, 2))
    plan = jnp.stack(
        [active.astype(jnp.int32), slot_lengths, jnp.full_like(steps, source), entry], axis=1
    ).astype(jnp.int32)
    fast, slow, sums = {}, {}, []
    for slot in range(slots):
        passed = [
            fast.get(slot - 1, query_states[0]),
            slow.get(slot - 2, query_states[0]),
        ]
        mixed = attention_half(
            slot, plan, query_states, doc_states, passed, attention_weights, groups, gain_attn
        )
        hidden, pool = mlp_half(slot, plan, mixed, mlp_weights, gain_mlp)
        sums.append(pool)
        for step, table in ((0, fast), (1, slow)):
            moves = [
                (index, index + 1)
                for index in range(step, section_count - 1, 2)
                if 0 <= slot - lag(index) < batch
            ]
            if moves:
                table[slot] = lax.ppermute(hidden, "pipe", moves)

    summed = jnp.concatenate(sums[slots - batch :], axis=0)
    own_lengths = lax.dynamic_slice_in_dim(lengths, host * batch, batch, 0)
    pooled = summed / own_lengths.astype(jnp.float32)[:, None]
    embedded = (
        pooled * lax.rsqrt(jnp.sum(pooled * pooled, axis=1, keepdims=True) + EPSILON)
    ).astype(jnp.bfloat16)
    embedded = jnp.where(is_host & (section == section_count - 1), embedded, jnp.zeros_like(embedded))
    table = lax.psum(lax.all_gather(embedded, "dp"), "pipe")
    table = jnp.where(
        jnp.arange(2, dtype=jnp.int32)[None, :, None, None] == host,
        table[:, None],
        jnp.zeros_like(table)[:, None],
    )
    table = lax.psum(table, "tensor").astype(jnp.bfloat16)
    table = table.reshape(dp_count, seq_count, model_width)
    mine = lax.dynamic_index_in_dim(table, dp_index, 0, keepdims=False)
    local_queries, local_docs = mine[:pair_count], mine[pair_count:]
    all_docs = table[:, pair_count:].reshape(dp_count * pair_count, model_width)
    scores = (
        lax.dot_general(
            local_queries,
            all_docs,
            (((1,), (1,)), ((), ())),
            preferred_element_type=jnp.float32,
        )
        / SOFTMAX_TEMPER
    )
    columns = jnp.arange(dp_count * pair_count, dtype=jnp.int32)
    positive = dp_index * pair_count + doc_order[0]
    positive_score = jnp.sum(
        jnp.where(columns[None, :] == positive[:, None], scores, 0.0), axis=1
    )
    pair_loss = jnp.log(jnp.sum(jnp.exp(scores), axis=1)) - positive_score
    piece_width = model_width // (section_count * tensor_count)
    first = (section * tensor_count + tensor_index) * piece_width
    return (
        lax.dynamic_slice_in_dim(local_queries, first, piece_width, 1),
        lax.dynamic_slice_in_dim(local_docs, first, piece_width, 1),
        pair_loss,
    )


def solution(mesh):
    in_specs = (
        P("dp", None, None),
        P("dp", None, None),
        P("dp"),
        P("dp"),
        P("dp", None),
        P("pipe", None, None, "tensor"),
        P("pipe", "tensor", None),
        P("pipe", None, "tensor"),
        P("pipe", "tensor", None),
        P("pipe", None),
        P("pipe", None),
    )
    out_specs = (P("dp", ("pipe", "tensor")), P("dp", ("pipe", "tensor")), P("dp"))
    return jax.shard_map(
        per_device, mesh=mesh, in_specs=in_specs, out_specs=out_specs, check_vma=False
    )
```
